8 devices in a mesh: data: 2 (over z, y), stage: 4 (over x, core).
Axes of the slice: x: 2, y: 2, z: 1, core: 2. Of those that a mesh axis runs over, the one named last changes fastest.
Arguments:
- x_in: bfloat16 [4, 4, 256, 2048], P(None, 'data')
- g_out: bfloat16 [4, 4, 256, 2048], P(None, 'data')
- w_gate: bfloat16 [4, 1, 2048, 8192], P('stage', None, 'data')
- w_in: bfloat16 [4, 1, 2048, 8192], P('stage', None, 'data')
- w_out: bfloat16 [4, 1, 8192, 2048], P('stage', None, 'data')
Outputs:
- output 1: bfloat16 [4, 4, 256, 2048], P(None, 'data')
- output 2: float32 [4, 1, 2048, 8192], P('stage', None, 'data')
- output 3: float32 [4, 1, 2048, 8192], P('stage', None, 'data')
- output 4: float32 [4, 1, 8192, 2048], P('stage', None, 'data')
All inputs are finite; a program needn't handle non-finite values.
Results may differ from the reference program's by a relative error of at most 0.0134286.
Values are sent between devices in bfloat16 or wider.
A program may use at most 1 GiB of HBM per device.

```python
import jax
import jax.numpy as jnp
from jax import lax

N_DATA = 2
N_STAGES = 4
LAYERS_STAGE = 1
D_MODEL = 2048
D_FF = 8192
MICRO_BATCHES = 4
BATCH_MICRO = 2
SEQ_LEN = 256
EPS = 1e-6


def setup_inputs(seed: int = 0) -> dict:
    key = jax.random.key(seed)
    k_x, k_g, k_gate, k_in, k_out = jax.random.split(key, 5)
    act_shape = (MICRO_BATCHES, N_DATA * BATCH_MICRO, SEQ_LEN, D_MODEL)
    up_shape = (N_STAGES, LAYERS_STAGE, D_MODEL, D_FF)
    down_shape = (N_STAGES, LAYERS_STAGE, D_FF, D_MODEL)
    x_in = jax.random.normal(k_x, act_shape, jnp.float32).astype(jnp.bfloat16)
    g_out = jax.random.normal(k_g, act_shape, jnp.float32).astype(jnp.bfloat16)
    w_gate = (jax.random.normal(k_gate, up_shape, jnp.float32) * D_MODEL ** -0.5).astype(jnp.bfloat16)
    w_in = (jax.random.normal(k_in, up_shape, jnp.float32) * D_MODEL ** -0.5).astype(jnp.bfloat16)
    w_out = (jax.random.normal(k_out, down_shape, jnp.float32) * (0.7 * D_FF ** -0.5)).astype(jnp.bfloat16)
    return {"x_in": x_in, "g_out": g_out, "w_gate": w_gate, "w_in": w_in, "w_out": w_out}


def rms_parts(h_rows):
    h_f32 = h_rows.astype(jnp.float32)
    inv_rms = lax.rsqrt(jnp.mean(h_f32 * h_f32, axis=-1, keepdims=True) + EPS)
    return h_f32 * inv_rms, inv_rms


def layer_forward(h_rows, gate_w, in_w, out_w):
    normed_f, inv_rms = rms_parts(h_rows)
    normed = normed_f.astype(jnp.bfloat16)
    gate_pre = jnp.dot(normed, gate_w, preferred_element_type=jnp.float32)
    up_pre = jnp.dot(normed, in_w, preferred_element_type=jnp.float32)
    act = (gate_pre * jax.nn.sigmoid(gate_pre) * up_pre).astype(jnp.bfloat16)
    branch = jnp.dot(act, out_w, preferred_element_type=jnp.float32)
    return h_rows + branch.astype(jnp.bfloat16)


def layer_backward(h_rows, d_out, gate_w, in_w, out_w):
    normed_f, inv_rms = rms_parts(h_rows)
    normed = normed_f.astype(jnp.bfloat16)
    gate_pre = jnp.dot(normed, gate_w, preferred_element_type=jnp.float32)
    up_pre = jnp.dot(normed, in_w, preferred_element_type=jnp.float32)
    gate_sig = jax.nn.sigmoid(gate_pre)
    silu_val = gate_pre * gate_sig
    act = (silu_val * up_pre).astype(jnp.bfloat16)
    d_act = jnp.dot(d_out, out_w.T, preferred_element_type=jnp.float32)
    d_out_w = jnp.dot(act.T, d_out, preferred_element_type=jnp.float32)
    d_gate = (d_act * up_pre * gate_sig * (1.0 + gate_pre * (1.0 - gate_sig))).astype(jnp.bfloat16)
    d_up = (d_act * silu_val).astype(jnp.bfloat16)
    d_gate_w = jnp.dot(normed.T, d_gate, preferred_element_type=jnp.float32)
    d_in_w = jnp.dot(normed.T, d_up, preferred_element_type=jnp.float32)
    d_norm = jnp.dot(d_gate, gate_w.T, preferred_element_type=jnp.float32) + jnp.dot(d_up, in_w.T, preferred_element_type=jnp.float32)
    d_res = inv_rms * (d_norm - normed_f * jnp.mean(d_norm * normed_f, axis=-1, keepdims=True))
    d_h = (d_out.astype(jnp.float32) + d_res).astype(jnp.bfloat16)
    return d_h, d_gate_w, d_in_w, d_out_w


def reference(x_in, g_out, w_gate, w_in, w_out):
    n_layers = N_STAGES * LAYERS_STAGE
    rows = N_DATA * BATCH_MICRO * SEQ_LEN
    gate_all = w_gate.reshape(n_layers, D_MODEL, D_FF)
    in_all = w_in.reshape(n_layers, D_MODEL, D_FF)
    out_all = w_out.reshape(n_layers, D_FF, D_MODEL)

    def fwd_step(h_cur, weights):
        gate_w, in_w, out_w = weights
        return layer_forward(h_cur, gate_w, in_w, out_w), h_cur

    def bwd_step(d_cur, layer_vals):
        h_saved, gate_w, in_w, out_w = layer_vals
        d_prev, d_gate_w, d_in_w, d_out_w = layer_backward(h_saved, d_cur, gate_w, in_w, out_w)
        return d_prev, (d_gate_w, d_in_w, d_out_w)

    def micro_step(grad_sums, pair):
        x_mb, g_mb = pair
        unused, saved = lax.scan(fwd_step, x_mb.reshape(rows, D_MODEL), (gate_all, in_all, out_all))
        d_first, layer_grads = lax.scan(bwd_step, g_mb.reshape(rows, D_MODEL), (saved, gate_all, in_all, out_all), reverse=True)
        new_sums = tuple(grad_sum + grad_new for grad_sum, grad_new in zip(grad_sums, layer_grads))
        return new_sums, d_first.reshape(x_mb.shape)

    zero_up = jnp.zeros((n_layers, D_MODEL, D_FF), jnp.float32)
    zero_down = jnp.zeros((n_layers, D_FF, D_MODEL), jnp.float32)
    grad_sums, dx_in = lax.scan(micro_step, (zero_up, zero_up, zero_down), (x_in, g_out))
    return (dx_in, grad_sums[0].reshape(w_gate.shape), grad_sums[1].reshape(w_in.shape), grad_sums[2].reshape(w_out.shape))
```

```python
import jax
import jax.numpy as jnp
from jax import lax
from jax.experimental import pallas as pl
from jax.experimental.pallas import tpu as pltpu
from jax.sharding import Mesh, PartitionSpec as P

EPS = 1e-6
BF16 = jnp.bfloat16
F32 = jnp.float32
VMEM_LIMIT = 60 * 2**20
AXES = ("data", "x", "core")


def dot_nn(left, right):
    return jnp.dot(left, right, preferred_element_type=F32)


def dot_nt(left, right):
    return lax.dot_general(left, right, (((1,), (1,)), ((), ())), preferred_element_type=F32)


def dot_tn(left, right):
    return lax.dot_general(left, right, (((0,), (0,)), ((), ())), preferred_element_type=F32)


def rms_parts(h_rows):
    h_f32 = h_rows.astype(F32)
    inv_rms = lax.rsqrt(jnp.mean(h_f32 * h_f32, axis=-1, keepdims=True) + EPS)
    return h_f32 * inv_rms, inv_rms


def fwd_kernel(scal, h_ref, g_ref, u_ref, o_ref, *refs):
    out_ref, a_ref, b_ref, s_ref, n_scr, acc = refs[-6:]
    tile = pl.program_id(0)
    tiles = pl.num_programs(0)

    @pl.when(scal[0] == 1)
    def _():
        @pl.when(tile == 0)
        def _():
            n_scr[...] = rms_parts(h_ref[...])[0].astype(BF16)
            acc[...] = jnp.zeros_like(acc)

        a = dot_nn(n_scr[...], g_ref[...])
        b = dot_nn(n_scr[...], u_ref[...])
        s = (a * jax.nn.sigmoid(a) * b).astype(BF16)
        a_ref[...] = a
        b_ref[...] = b

        @pl.when((tile >= tiles // 2) == (scal[1] == 1))
        def _():
            s_ref[...] = s

        acc[...] += dot_nn(s, o_ref[...])

        @pl.when(tile == tiles - 1)
        def _():
            out_ref[...] = h_ref[...] + acc[...].astype(BF16)


def fwd_call(scal, h_rows, gate_w, in_w, out_w, saved, tile_w=512):
    rows, d_model = h_rows.shape
    d_ff = gate_w.shape[1]
    tiles = d_ff // tile_w
    half = tiles // 2
    whole = pl.BlockSpec((rows, d_model), lambda j, sc: (0, 0))
    wide = pl.BlockSpec((rows, tile_w), lambda j, sc: (sc[2], j * sc[0]))
    s_spec = pl.BlockSpec((rows, tile_w), lambda j, sc: (sc[3], jnp.clip(j - sc[1] * half, 0, half - 1) * sc[0]))
    up_spec = pl.BlockSpec((d_model, tile_w), lambda j, sc: (0, j * sc[0]))
    down_spec = pl.BlockSpec((tile_w, d_model), lambda j, sc: (j * sc[0], 0))
    extra = [] if saved is None else list(saved)
    aliases = {} if saved is None else {5: 1, 6: 2, 7: 3}
    return pl.pallas_call(
        fwd_kernel,
        grid_spec=pltpu.PrefetchScalarGridSpec(
            num_scalar_prefetch=1,
            grid=(tiles,),
            in_specs=[whole, up_spec, up_spec, down_spec] + [pl.BlockSpec(memory_space=pl.ANY)] * len(extra),
            out_specs=[whole, wide, wide, s_spec],
            scratch_shapes=[pltpu.VMEM((rows, d_model), BF16), pltpu.VMEM((rows, d_model), F32)],
        ),
        out_shape=[
            jax.ShapeDtypeStruct((rows, d_model), BF16),
            jax.ShapeDtypeStruct((5 * rows, d_ff), F32),
            jax.ShapeDtypeStruct((5 * rows, d_ff), F32),
            jax.ShapeDtypeStruct((5 * rows, d_ff // 2), BF16),
        ],
        input_output_aliases=aliases,
        compiler_params=pltpu.CompilerParams(dimension_semantics=("arbitrary",), vmem_limit_bytes=VMEM_LIMIT),
        cost_estimate=pl.CostEstimate(flops=6 * rows * d_model * d_ff, bytes_accessed=6 * d_model * d_ff, transcendentals=0),
        name="block_forward",
    )(scal, h_rows, gate_w, in_w, out_w, *extra)


def bwd_kernel(scal, e_ref, h_ref, a_ref, b_ref, g_ref, u_ref, o_ref, *refs):
    out_ref, da_ref, db_ref, acc = refs[-4:]
    tile = pl.program_id(0)

    @pl.when(scal[0] == 1)
    def _():
        @pl.when(tile == 0)
        def _():
            acc[...] = jnp.zeros_like(acc)

        a = a_ref[...]
        b = b_ref[...]
        t = dot_nt(e_ref[...], o_ref[...])
        sig = jax.nn.sigmoid(a)
        da = (t * b * sig * (1.0 + a * (1.0 - sig))).astype(BF16)
        db = (t * (a * sig)).astype(BF16)
        da_ref[...] = da
        db_ref[...] = db
        acc[...] += dot_nt(da, g_ref[...]) + dot_nt(db, u_ref[...])

        @pl.when(tile == pl.num_programs(0) - 1)
        def _():
            normed, inv_rms = rms_parts(h_ref[...])
            q = acc[...]
            d_res = inv_rms * (q - normed * jnp.mean(q * normed, axis=-1, keepdims=True))
            out_ref[...] = (e_ref[...].astype(F32) + d_res).astype(BF16)


def bwd_call(scal, e_rows, h_rows, a_all, b_all, gate_w, in_w, out_w, grads, tile_w=512):
    rows, d_model = h_rows.shape
    d_ff = gate_w.shape[1]
    tiles = d_ff // tile_w
    whole = pl.BlockSpec((rows, d_model), lambda j, sc: (0, 0))
    ab_spec = pl.BlockSpec((rows, tile_w), lambda j, sc: (sc[2], j * sc[0]))
    grad_spec = pl.BlockSpec((rows, tile_w), lambda j, sc: (sc[3], j * sc[0]))
    up_spec = pl.BlockSpec((d_model, tile_w), lambda j, sc: (0, j * sc[0]))
    down_spec = pl.BlockSpec((tile_w, d_model), lambda j, sc: (j * sc[0], 0))
    extra = [] if grads is None else list(grads)
    aliases = {} if grads is None else {8: 1, 9: 2}
    return pl.pallas_call(
        bwd_kernel,
        grid_spec=pltpu.PrefetchScalarGridSpec(
            num_scalar_prefetch=1,
            grid=(tiles,),
            in_specs=[whole, whole, ab_spec, ab_spec, up_spec, up_spec, down_spec] + [pl.BlockSpec(memory_space=pl.ANY)] * len(extra),
            out_specs=[whole, grad_spec, grad_spec],
            scratch_shapes=[pltpu.VMEM((rows, d_model), F32)],
        ),
        out_shape=[
            jax.ShapeDtypeStruct((rows, d_model), BF16),
            jax.ShapeDtypeStruct((5 * rows, d_ff), BF16),
            jax.ShapeDtypeStruct((5 * rows, d_ff), BF16),
        ],
        input_output_aliases=aliases,
        compiler_params=pltpu.CompilerParams(dimension_semantics=("arbitrary",), vmem_limit_bytes=VMEM_LIMIT),
        cost_estimate=pl.CostEstimate(flops=6 * rows * d_model * d_ff, bytes_accessed=6 * d_model * d_ff, transcendentals=0),
        name="block_backward",
    )(scal, e_rows, h_rows, a_all, b_all, gate_w, in_w, out_w, *extra)


def redo_kernel(scal, n_ref, e_ref, g_ref, u_ref, o_ref, da_ref, db_ref, s_ref):
    tile = pl.program_id(1)
    a = dot_nn(n_ref[...], g_ref[...])
    b = dot_nn(n_ref[...], u_ref[...])
    t = dot_nt(e_ref[...], o_ref[...])
    sig = jax.nn.sigmoid(a)
    silu = a * sig

    @pl.when((tile >= pl.num_programs(1) // 2) == (scal[0] == 1))
    def _():
        s_ref[...] = (silu * b).astype(BF16)

    da_ref[...] = (t * b * sig * (1.0 + a * (1.0 - sig))).astype(BF16)
    db_ref[...] = (t * silu).astype(BF16)


def redo_call(scal, n_rows, e_rows, gate_w, in_w, out_w, row_block=1024, tile_w=512):
    rows, d_model = n_rows.shape
    d_ff = gate_w.shape[1]
    tiles = d_ff // tile_w
    half = tiles // 2
    row_spec = pl.BlockSpec((row_block, d_model), lambda i, j, sc: (i, 0))
    wide = pl.BlockSpec((row_block, tile_w), lambda i, j, sc: (i, j))
    s_spec = pl.BlockSpec((row_block, tile_w), lambda i, j, sc: (i, jnp.clip(j - sc[0] * half, 0, half - 1)))
    up_spec = pl.BlockSpec((d_model, tile_w), lambda i, j, sc: (0, j))
    down_spec = pl.BlockSpec((tile_w, d_model), lambda i, j, sc: (j, 0))
    return pl.pallas_call(
        redo_kernel,
        grid_spec=pltpu.PrefetchScalarGridSpec(
            num_scalar_prefetch=1,
            grid=(rows // row_block, tiles),
            in_specs=[row_spec, row_spec, up_spec, up_spec, down_spec],
            out_specs=[wide, wide, s_spec],
        ),
        out_shape=[
            jax.ShapeDtypeStruct((rows, d_ff), BF16),
            jax.ShapeDtypeStruct((rows, d_ff), BF16),
            jax.ShapeDtypeStruct((rows, d_ff // 2), BF16),
        ],
        compiler_params=pltpu.CompilerParams(dimension_semantics=("arbitrary", "arbitrary"), vmem_limit_bytes=VMEM_LIMIT),
        cost_estimate=pl.CostEstimate(flops=6 * rows * d_model * d_ff, bytes_accessed=6 * d_model * d_ff, transcendentals=0),
        name="block_redo",
    )(scal, n_rows, e_rows, gate_w, in_w, out_w)


def pair_list(keep, move):
    pairs = []
    for data in range(2):
        for x in range(2):
            for core in range(2):
                if keep(data, x, core):
                    to = move(data, x, core)
                    pairs.append((data * 4 + x * 2 + core, to[0] * 4 + to[1] * 2 + to[2]))
    return pairs


EVERY = lambda d, x, c: True
CORE_SWAP = pair_list(EVERY, lambda d, x, c: (d, x, 1 - c))
DATA_SWAP = pair_list(EVERY, lambda d, x, c: (1 - d, x, c))
DIAG_SWAP = pair_list(EVERY, lambda d, x, c: (1 - d, x, 1 - c))
HOP_UP = pair_list(lambda d, x, c: x == 0, lambda d, x, c: (d, 1, c))
HOP_DOWN = pair_list(lambda d, x, c: x == 1, lambda d, x, c: (d, 0, c))


def move(value, pairs):
    return lax.ppermute(value, AXES, pairs)


def solution(mesh):
    mesh3 = Mesh(mesh.devices.reshape(2, 2, 2), AXES)

    def body(x_loc, g_loc, gate_loc, in_loc, out_loc):
        data = lax.axis_index("data")
        x_pos = lax.axis_index("x")
        core = lax.axis_index("core")
        low = x_pos == 0
        n_micro, batch, seq, d_model = x_loc.shape
        d_ff = gate_loc.shape[-1]
        per_core = n_micro * batch * seq // 2
        chunks = 2
        rows = per_core // chunks

        def pieces(shard):
            half = shard.shape[0] // 2
            mine = lax.dynamic_slice_in_dim(shard, core * half, half, 0)
            other = lax.dynamic_slice_in_dim(shard, (1 - core) * half, half, 0)
            got = move(other, CORE_SWAP)
            return [jnp.where(core == block, mine, got) for block in range(2)]

        parts = [pieces(w[0, 0]) for w in (gate_loc, in_loc, out_loc)]
        weights = [[lax.all_gather(parts[w][block], ("data", "core"), axis=0, tiled=True) for w in range(3)] for block in range(2)]

        x_rows = lax.dynamic_index_in_dim(x_loc, core, 1, keepdims=False).reshape(chunks, rows, d_model)
        g_rows = lax.dynamic_index_in_dim(g_loc, core, 1, keepdims=False).reshape(chunks, rows, d_model)

        def scal_of(valid, block, chunk):
            role = jnp.where(core == block, 0, 1)
            ab_row = jnp.where(valid, block * chunks + chunk, 2 * chunks)
            role_row = jnp.where(valid, role * chunks + chunk, 2 * chunks)
            return jnp.stack([valid.astype(jnp.int32), data, ab_row, role_row]).astype(jnp.int32)

        saved = None
        grads = None

        def forward(valid, block, chunk, h_rows):
            nonlocal saved
            out, *saved = fwd_call(scal_of(valid, block, chunk), h_rows, *weights[block], saved)
            return out

        def backward(valid, block, chunk, e_rows, h_rows):
            nonlocal grads
            out, *grads = bwd_call(scal_of(valid, block, chunk), e_rows, h_rows, saved[0], saved[1], *weights[block], grads)
            return out

        high = jnp.logical_not(low)
        mid_low = [forward(low, 0, ch, x_rows[ch]) for ch in range(chunks)]
        got_up = []
        for ch in range(chunks):
            got_up.append(move(forward(low, 1, ch, mid_low[ch]), HOP_UP))
        h_in = [[None] * chunks, [None] * chunks]
        e_out = [[None] * chunks, [None] * chunks]
        for ch in range(chunks):
            mid = forward(high, 0, ch, got_up[ch])
            forward(high, 1, ch, mid)
            h_in[0][ch] = jnp.where(low, x_rows[ch], got_up[ch])
            h_in[1][ch] = jnp.where(low, mid_low[ch], mid)
        got_down = []
        mid_high = []
        for ch in range(chunks):
            e_mid = backward(high, 1, ch, g_rows[ch], h_in[1][ch])
            mid_high.append(e_mid)
            got_down.append(move(backward(high, 0, ch, e_mid, h_in[0][ch]), HOP_DOWN))
        dx = []
        for ch in range(chunks):
            e_mid = backward(low, 1, ch, got_down[ch], h_in[1][ch])
            dx.append(backward(low, 0, ch, e_mid, h_in[0][ch]))
            e_out[1][ch] = jnp.where(low, got_down[ch], g_rows[ch])
            e_out[0][ch] = jnp.where(low, e_mid, mid_high[ch])

        full = []
        for ch in range(chunks):
            here = jnp.where(low, dx[ch], move(dx[ch], HOP_UP))
            there = move(here, CORE_SWAP)
            pair = jnp.where(core == 0, jnp.stack([here, there]), jnp.stack([there, here]))
            full.append(pair.reshape(batch, n_micro // chunks, seq, d_model).swapaxes(0, 1))
        dx_all = jnp.concatenate(full, axis=0)

        def exchange(values):
            same, cross = [], []
            for ch in range(chunks):
                own = jnp.where(core == 0, values[0][ch], values[1][ch])
                sib = jnp.where(core == 0, values[1][ch], values[0][ch])
                same.append(move(own, DATA_SWAP))
                cross.append(move(sib, DIAG_SWAP))
            return jnp.concatenate(same + cross, axis=0)

        def own_side(values):
            own = jnp.concatenate([jnp.where(core == 0, values[0][ch], values[1][ch]) for ch in range(chunks)], axis=0)
            sib = jnp.concatenate([jnp.where(core == 0, values[1][ch], values[0][ch]) for ch in range(chunks)], axis=0)
            return own, move(sib, CORE_SWAP)

        h_far = exchange(h_in)
        e_far = exchange(e_out)
        n_far = rms_parts(h_far)[0].astype(BF16)
        redo_scal = jnp.stack([data]).astype(jnp.int32)
        da_far, db_far, s_far = lax.cond(
            core == 0,
            lambda: tuple(redo_call(redo_scal, n_far, e_far, *weights[0])),
            lambda: tuple(redo_call(redo_scal, n_far, e_far, *weights[1])),
        )

        h_own, h_sib = own_side(h_in)
        e_own, e_sib = own_side(e_out)
        da_all, db_all = grads
        s_all = saved[2]

        def split(stacked):
            return stacked[:per_core], move(stacked[per_core:2 * per_core], CORE_SWAP)

        da_own, da_sib = split(da_all)
        db_own, db_sib = split(db_all)
        s_own, s_sib = split(s_all)
        col = d_model // 2

        def half_cols(normed):
            return lax.dynamic_slice_in_dim(normed, data * col, col, 1)

        n_own = half_cols(rms_parts(h_own)[0].astype(BF16))
        n_sib = half_cols(rms_parts(h_sib)[0].astype(BF16))
        n_far = half_cols(n_far)

        def weight_grad(lefts, rights):
            left = jnp.concatenate(lefts, axis=0)
            right = jnp.concatenate(rights, axis=0)
            return dot_tn(left, right)

        lefts = [n_own, n_sib, n_far]
        gate_grad = weight_grad(lefts, [da_own, da_sib, da_far])
        in_grad = weight_grad(lefts, [db_own, db_sib, db_far])
        out_grad = weight_grad([s_own, s_sib, s_far], [e_own, e_sib, e_far])
        return dx_all, gate_grad[None, None], in_grad[None, None], out_grad[None, None]

    act_spec = P(None, "data", None, None)
    weight_spec = P(("x", "core"), None, "data", None)
    return jax.shard_map(
        body,
        mesh=mesh3,
        in_specs=(act_spec, act_spec, weight_spec, weight_spec, weight_spec),
        out_specs=(act_spec, weight_spec, weight_spec, weight_spec),
        check_vma=False,
    )
```
